32 devices in a mesh: row: 8 (over z, x), col: 4 (over y, core).
Axes of the slice: x: 2, y: 2, z: 4, core: 2. Of those that a mesh axis runs over, the one named last changes fastest.
Arguments:
- tokens: bfloat16 [64, 12288], P('row', 'col'), may hold values from -6 to 6
- past_tokens: bfloat16 [64, 12288], P('row', 'col'), may hold values from -6 to 6
- out_grad: bfloat16 [64, 12288], P('row', 'col'), may hold values from -3 to 3
- w_in: bfloat16 [12288, 24576], P('col', 'row'), may hold values from -0.0546875 to 0.0546875
- w_out: bfloat16 [24576, 12288], P('row', 'col'), may hold values from -0.0390625 to 0.0390625
Outputs:
- layer_out: bfloat16 [64, 12288], P('row', 'col')
- input_grad: bfloat16 [64, 12288], P('row', 'col')
- grad_w_in: bfloat16 [12288, 24576], P('col', 'row')
- grad_w_out: bfloat16 [24576, 12288], P('row', 'col')
The draws below stay inside these ranges and needn't reach their ends.
All inputs are finite; a program needn't handle non-finite values.
Results may differ from the reference program's by a relative error of at most 0.005.
Values may be sent and summed in bfloat16 or wider, within the bound.
A program may use at most 128 MiB of HBM per device.

```python
import jax
import jax.numpy as jnp

D = 12288
FF = 24576
TOKENS = 64


def steps_of(rng, extent, pieces, least, high):
    level, own = 1.0, jax.random.fold_in(rng, 6)
    for position, parts in pieces:
        draws = jnp.exp(jax.random.uniform(jax.random.fold_in(own, position), (parts,), jnp.float32, least / len(pieces), high / len(pieces)))
        level = level * jnp.repeat(draws, extent[position] // parts).reshape([-1 if axis == position else 1 for axis in range(len(extent))])
    return level


def centred(own_key, shape, spread, reach, shards=(), kind=jnp.bfloat16):
    result = jax.random.normal(own_key, shape, jnp.float32) * spread
    if len(shards) > 0:
        result = steps_of(own_key, shape, shards, -0.22, 0.18) * result
    return jnp.clip(result, min=-reach, max=reach).astype(kind)


def setup_inputs(seed: int = 0) -> dict:
    streams_of = jax.random.split(jax.random.key(seed), 6)
    tokens = centred(streams_of[0], (TOKENS, D), 1.0, 6.0, ((0, 8), (1, 4)))
    past_tokens = centred(streams_of[1], (TOKENS, D), 1.0, 6.0, ((0, 8), (1, 4)))
    out_grad = centred(streams_of[2], (TOKENS, D), 0.5, 3.0, ((0, 8), (1, 4)))
    w_in = centred(streams_of[3], (D, FF), D ** -0.5, 0.0546875, ((0, 4), (1, 8)))
    w_out = centred(streams_of[4], (FF, D), FF ** -0.5, 0.0390625, ((0, 8), (1, 4)))
    return {"tokens": tokens, "past_tokens": past_tokens, "out_grad": out_grad, "w_in": w_in, "w_out": w_out}


def gelu_parts(pre):
    cdf = 0.5 * (1.0 + jax.scipy.special.erf(pre * 0.7071067811865476))
    slope = cdf + pre * jnp.exp(-0.5 * pre * pre) * 0.3989422804014327
    return pre * cdf, slope


def reference(tokens, past_tokens, out_grad, w_in, w_out):
    pre = jnp.dot(tokens, w_in, preferred_element_type=jnp.float32)
    hidden = gelu_parts(pre)[0].astype(jnp.bfloat16)
    layer_out = jnp.dot(hidden, w_out, preferred_element_type=jnp.float32).astype(jnp.bfloat16)
    past_pre = jnp.dot(past_tokens, w_in, preferred_element_type=jnp.float32)
    past_act, slope = gelu_parts(past_pre)
    past_hidden = past_act.astype(jnp.bfloat16)
    back = jnp.dot(out_grad, w_out.T, preferred_element_type=jnp.float32)
    hidden_grad = (back * slope).astype(jnp.bfloat16)
    grad_w_out = jnp.dot(past_hidden.T, out_grad, preferred_element_type=jnp.float32).astype(jnp.bfloat16)
    grad_w_in = jnp.dot(past_tokens.T, hidden_grad, preferred_element_type=jnp.float32).astype(jnp.bfloat16)
    input_grad = jnp.dot(hidden_grad, w_in.T, preferred_element_type=jnp.float32).astype(jnp.bfloat16)
    return layer_out, input_grad, grad_w_in, grad_w_out
```

```python
import functools

import jax
import jax.numpy as jnp
from jax import lax
from jax.experimental import pallas as pl
from jax.experimental.pallas import tpu as pltpu
from jax.sharding import PartitionSpec as P

MESH = pl.DeviceIdType.MESH
F32, BF16 = jnp.float32, jnp.bfloat16
NN = (((1,), (0,)), ((), ()))
NT = (((1,), (1,)), ((), ()))
TN = (((0,), (0,)), ((), ()))


def cdf_of(v):
    return 0.5 * (1.0 + lax.erf(v * 0.7071067811865476))


def slope_of(v, cdf):
    return cdf + v * jnp.exp(-0.5 * v * v) * 0.3989422804014327


def cols(i, width):
    return pl.ds(pl.multiple_of(i * width, width), width)


def exchange_kernel(
    nr, nc, nck,
    past_ref, grad_ref, tok_ref, win_hbm, wout_hbm,
    xpast, xgrad, act_out, hg_out, out_lo, out_ig,
    win, wout, g_past, g_grad, g_tok, xtok, hid,
    part, pair_in, y_out, y_in, halves,
    rs_all, rs_xs, rs_xr, rs_zs, rs_zr,
    win_sem, wout_sem, up_s, up_r, dn_s, dn_r, gx_s, gx_r,
    pr_s, pr_r, y_s, y_r, hv_s, hv_r, rx_s, rx_r, rz_s, rz_r,
):
    me, col = lax.axis_index("row"), lax.axis_index("col")
    nh, ny = nr // 2, nc // 2
    h, lo = me // 2, me % 2
    g, core = col // 2, col % 2
    d, ff = win.shape
    tr = past_ref.shape[0]
    t = nr * tr
    cw, dw = ff // nck, d // nck
    partner = (h * 2 + 1 - lo, col)
    mate = (me, g * 2 + 1 - core)

    def zdev(k):
        return (k * 2 + lo, col)

    def ydev(k):
        return (me, k * 2 + core)

    def rcopy(src, dst, ss, rs, dev):
        return pltpu.make_async_remote_copy(
            src_ref=src, dst_ref=dst, send_sem=ss, recv_sem=rs, device_id=dev, device_id_type=MESH
        )

    def wout_copy(i):
        s = cols(i, cw)
        return pltpu.make_async_copy(wout_hbm.at[s, :], wout.at[s, :], wout_sem.at[i])

    def win_copy(i):
        s = cols(i, cw)
        return pltpu.make_async_copy(win_hbm.at[:, s], win.at[:, s], win_sem.at[i])

    for i in range(nck):
        wout_copy(i).start()
        win_copy(i).start()

    barrier = pltpu.get_barrier_semaphore()
    for q in range(1, nh):
        pl.semaphore_signal(barrier, inc=1, device_id=zdev((h + q) % nh), device_id_type=MESH)
    for q in range(1, ny):
        pl.semaphore_signal(barrier, inc=1, device_id=ydev((g + q) % ny), device_id_type=MESH)
    pl.semaphore_signal(barrier, inc=1, device_id=partner, device_id_type=MESH)
    pl.semaphore_signal(barrier, inc=1, device_id=mate, device_id_type=MESH)
    pl.semaphore_wait(barrier, nh + ny)

    owns = (past_ref, grad_ref, tok_ref)
    gath = (g_past, g_grad, g_tok)

    def up(a, s, src, blk):
        return rcopy(src, gath[a].at[blk], up_s.at[a, s], up_r.at[a, s], zdev(jnp.minimum(h + 1, nh - 1)))

    def down(a, s, src, blk):
        return rcopy(src, gath[a].at[blk], dn_s.at[a, s], dn_r.at[a, s], zdev(jnp.maximum(h - 1, 0)))

    def across(a, k, src, blk):
        return rcopy(src, gath[a].at[blk], gx_s.at[a, k], gx_r.at[a, k], partner)

    def start_own(a):
        across(a, h, owns[a], me).start()

        @pl.when(h < nh - 1)
        def _():
            up(a, 0, owns[a], me).start()

        @pl.when(h > 0)
        def _():
            down(a, 0, owns[a], me).start()

        gath[a][me] = owns[a][...]

    def relay(a, s):
        kb = h - 1 - s

        @pl.when(kb >= 0)
        def _():
            blk = kb * 2 + lo
            src = gath[a].at[blk]
            up(a, s, src, blk).wait_recv()

            @pl.when((h < nh - 1) & (s < nh - 2))
            def _():
                up(a, jnp.minimum(s + 1, nh - 2), src, blk).start()

            across(a, kb, src, blk).start()

        ka = h + 1 + s

        @pl.when(ka <= nh - 1)
        def _():
            blk = ka * 2 + lo
            src = gath[a].at[blk]
            down(a, s, src, blk).wait_recv()

            @pl.when((h > 0) & (s < nh - 2))
            def _():
                down(a, jnp.minimum(s + 1, nh - 2), src, blk).start()

            across(a, ka, src, blk).start()

    def collect(a, x):
        def wait_one(k, _):
            blk = k * 2 + 1 - lo
            across(a, k, gath[a].at[blk], blk).wait_recv()
            return 0

        lax.fori_loop(0, nh, wait_one, 0)

        def put(i, _):
            s = cols(i, dw)
            x[:, s] = gath[a][:, :, s].astype(F32).reshape(t, dw).astype(BF16)
            return 0

        lax.fori_loop(0, nck, put, 0)

    start_own(0)
    start_own(1)
    for s in range(nh - 1):
        relay(0, s)
        relay(1, s)
    start_own(2)
    collect(0, xpast)
    collect(1, xgrad)

    def pair_copy(a, i, half):
        return rcopy(part.at[a, i, half], pair_in.at[a, i], pr_s.at[a, i], pr_r.at[a, i], mate)

    def y_copy(a, i, q):
        return rcopy(
            y_out.at[a, i], y_in.at[a, i, q - 1], y_s.at[a, i, q - 1], y_r.at[a, i, q - 1], ydev((g + q) % ny)
        )

    def pair_add(a, j):
        pair_copy(a, j, 1 - core).wait_recv()
        total = part[a, j, core] + pair_in[a, j]
        part[a, j, core] = total
        y_out[a, j] = total.astype(BF16)

    def y_start(a, j):
        for q in range(1, ny):
            y_copy(a, j, q).start()

    def y_total(a, j):
        total = part[a, j, core]
        for q in range(1, ny):
            y_copy(a, j, q).wait_recv()
            total = total + y_in[a, j, q - 1].astype(F32)
        return total

    per = -(-(nh - 1) // nck)

    def back_step(i, _):
        @pl.when(i < nck)
        def _():
            s = cols(i, cw)
            wout_copy(i).wait()
            back = lax.dot_general(xgrad[...], wout[s, :], NT, preferred_element_type=F32)
            part[0, i] = back.reshape(2, t // 2, cw)
            win_copy(i).wait()
            past = lax.dot_general(xpast[...], win[:, s], NN, preferred_element_type=F32)
            part[1, i] = past.reshape(2, t // 2, cw)
            pair_copy(0, i, 1 - core).start()
            pair_copy(1, i, 1 - core).start()
            for k in range(per):
                @pl.when(i * per + k < nh - 1)
                def _():
                    relay(2, i * per + k)

        @pl.when(i > 0)
        def _():
            pair_add(0, i - 1)
            pair_add(1, i - 1)
            y_start(0, i - 1)
            y_start(1, i - 1)

        return 0

    lax.fori_loop(0, nck + 1, back_step, 0)
    collect(2, xtok)

    def fwd_step(i, _):
        @pl.when(i < nck)
        def _():
            s = cols(i, cw)
            pre = lax.dot_general(xtok[...], win[:, s], NN, preferred_element_type=F32)
            part[2, i] = pre.reshape(2, t // 2, cw)
            pair_copy(2, i, 1 - core).start()

        @pl.when(i > 0)
        def _():
            pair_add(2, i - 1)
            y_start(2, i - 1)

        return 0

    lax.fori_loop(0, nck + 1, fwd_step, 0)

    def half_copy(a, i, k):
        return rcopy(halves.at[a, i, k], halves.at[a, i, k], hv_s.at[a, i], hv_r.at[a, i], mate)

    def back_final(j, _):
        back = y_total(0, j)
        v = y_total(1, j)
        cdf = cdf_of(v)
        halves[0, j, core] = (v * cdf).astype(BF16)
        halves[1, j, core] = (back * slope_of(v, cdf)).astype(BF16)
        half_copy(1, j, core).start()
        half_copy(0, j, core).start()
        return 0

    lax.fori_loop(0, nck, back_final, 0)

    def land(a, dst):
        def one(j, _):
            half_copy(a, j, 1 - core).wait_recv()
            dst[:, cols(j, cw)] = halves[a, j].reshape(t, cw)
            return 0

        lax.fori_loop(0, nck, one, 0)

    land(1, hg_out)

    def rx_copy(o, i):
        return rcopy(rs_xs.at[o, i], rs_xr.at[o, i], rx_s.at[o, i], rx_r.at[o, i], partner)

    def rz_copy(o, i, q):
        k = (h + q) % nh
        return rcopy(rs_zs.at[o, i, k], rs_zr.at[o, i, q - 1], rz_s.at[o, i, q - 1], rz_r.at[o, i, q - 1], zdev(k))

    def rs_loop(o, product):
        def step(i, _):
            @pl.when(i < nck)
            def _():
                rs_all[o, i] = product(i).reshape(nh, 2, tr, dw)
                rs_xs[o, i] = rs_all[o, i, :, 1 - lo].astype(BF16)
                rx_copy(o, i).start()

            @pl.when(i > 0)
            def _():
                j = i - 1
                rx_copy(o, j).wait_recv()
                total = rs_all[o, j, :, lo] + rs_xr[o, j].astype(F32)
                rs_all[o, j, :, lo] = total
                rs_zs[o, j] = total.astype(BF16)
                for q in range(1, nh):
                    rz_copy(o, j, q).start()

            return 0

        lax.fori_loop(0, nck + 1, step, 0)

    rs_loop(0, lambda i: lax.dot_general(hg_out[...], win[cols(i, dw), :], NT, preferred_element_type=F32))

    def fwd_final(j, _):
        v = y_total(2, j)
        halves[2, j, core] = (v * cdf_of(v)).astype(BF16)
        half_copy(2, j, core).start()
        return 0

    lax.fori_loop(0, nck, fwd_final, 0)
    land(2, hid)
    rs_loop(1, lambda i: lax.dot_general(hid[...], wout[:, cols(i, dw)], NN, preferred_element_type=F32))
    land(0, act_out)

    def rs_final(o, out):
        def one(j, _):
            total = rs_all[o, j, h, lo]
            for q in range(1, nh):
                rz_copy(o, j, q).wait_recv()
                total = total + rs_zr[o, j, q - 1].astype(F32)
            out[:, cols(j, dw)] = total.astype(BF16)
            return 0

        lax.fori_loop(0, nck, one, 0)

    rs_final(0, out_ig)
    rs_final(1, out_lo)

    def drain(i, _):
        for a in range(3):
            pair_copy(a, i, 1 - core).wait_send()
            half_copy(a, i, core).wait_send()
            for q in range(1, ny):
                y_copy(a, i, q).wait_send()
        for o in range(2):
            rx_copy(o, i).wait_send()
            for q in range(1, nh):
                rz_copy(o, i, q).wait_send()
        return 0

    lax.fori_loop(0, nck, drain, 0)
    for a in range(3):
        def drain_across(k, _):
            across(a, k, owns[a], me).wait_send()
            return 0

        lax.fori_loop(0, nh, drain_across, 0)
        for s in range(nh - 1):
            @pl.when((h < nh - 1) & (h - s >= 0))
            def _():
                up(a, s, owns[a], me).wait_send()

            @pl.when((h > 0) & (h + s <= nh - 1))
            def _():
                down(a, s, owns[a], me).wait_send()


def grads_kernel(act, grad, past, hg, gwo, gwi):
    gwo[...] = lax.dot_general(act[...], grad[...], TN, preferred_element_type=F32).astype(BF16)
    gwi[...] = lax.dot_general(past[...], hg[...], TN, preferred_element_type=F32).astype(BF16)


def local(nr, nc, tokens, past_tokens, out_grad, w_in, w_out):
    d, ff = w_in.shape
    tr = tokens.shape[0]
    t, nh, ny, nck = nr * tr, nr // 2, nc // 2, 6
    cw, dw = ff // nck, d // nck
    dma = pltpu.SemaphoreType.DMA
    vm = pl.BlockSpec(memory_space=pltpu.VMEM)
    hbm = pl.BlockSpec(memory_space=pl.ANY)
    q = max(ny - 1, 1)
    past_all, grad_all, act_all, hg_all, lo, ig = pl.pallas_call(
        functools.partial(exchange_kernel, nr, nc, nck),
        out_shape=[
            jax.ShapeDtypeStruct((t, d), BF16),
            jax.ShapeDtypeStruct((t, d), BF16),
            jax.ShapeDtypeStruct((t, ff), BF16),
            jax.ShapeDtypeStruct((t, ff), BF16),
            jax.ShapeDtypeStruct((tr, d), BF16),
            jax.ShapeDtypeStruct((tr, d), BF16),
        ],
        in_specs=[vm, vm, vm, hbm, hbm],
        out_specs=[vm] * 6,
        scratch_shapes=[
            pltpu.VMEM((d, ff), BF16),
            pltpu.VMEM((ff, d), BF16),
            pltpu.VMEM((nr, tr, d), BF16),
            pltpu.VMEM((nr, tr, d), BF16),
            pltpu.VMEM((nr, tr, d), BF16),
            pltpu.VMEM((t, d), BF16),
            pltpu.VMEM((t, ff), BF16),
            pltpu.VMEM((3, nck, 2, t // 2, cw), F32),
            pltpu.VMEM((3, nck, t // 2, cw), F32),
            pltpu.VMEM((3, nck, t // 2, cw), BF16),
            pltpu.VMEM((3, nck, q, t // 2, cw), BF16),
            pltpu.VMEM((3, nck, 2, t // 2, cw), BF16),
            pltpu.VMEM((2, nck, nh, 2, tr, dw), F32),
            pltpu.VMEM((2, nck, nh, tr, dw), BF16),
            pltpu.VMEM((2, nck, nh, tr, dw), BF16),
            pltpu.VMEM((2, nck, nh, tr, dw), BF16),
            pltpu.VMEM((2, nck, nh - 1, tr, dw), BF16),
            dma((nck,)), dma((nck,)),
            dma((3, nh - 1)), dma((3, nh - 1)), dma((3, nh - 1)), dma((3, nh - 1)),
            dma((3, nh)), dma((3, nh)),
            dma((3, nck)), dma((3, nck)),
            dma((3, nck, q)), dma((3, nck, q)),
            dma((3, nck)), dma((3, nck)),
            dma((2, nck)), dma((2, nck)),
            dma((2, nck, nh - 1)), dma((2, nck, nh - 1)),
        ],
        compiler_params=pltpu.CompilerParams(
            collective_id=0, has_side_effects=True, vmem_limit_bytes=66 * 1000 * 1000
        ),
    )(past_tokens, out_grad, tokens, w_in, w_out)

    tile = 128
    gwo, gwi = pl.pallas_call(
        grads_kernel,
        grid=(ff // tile,),
        out_shape=[jax.ShapeDtypeStruct((ff, d), BF16), jax.ShapeDtypeStruct((d, ff), BF16)],
        in_specs=[
            pl.BlockSpec((t, tile), lambda i: (0, i)),
            pl.BlockSpec((t, d), lambda i: (0, 0)),
            pl.BlockSpec((t, d * tile // ff), lambda i: (0, i)),
            pl.BlockSpec((t, ff), lambda i: (0, 0)),
        ],
        out_specs=[
            pl.BlockSpec((tile, d), lambda i: (i, 0)),
            pl.BlockSpec((d * tile // ff, ff), lambda i: (i, 0)),
        ],
        cost_estimate=pl.CostEstimate(flops=4 * t * d * ff, bytes_accessed=4 * d * ff, transcendentals=0),
    )(act_all, grad_all, past_all, hg_all)
    return lo, ig, gwi, gwo


def solution(mesh):
    nr, nc = mesh.shape["row"], mesh.shape["col"]
    in_specs = (P("row", "col"), P("row", "col"), P("row", "col"), P("col", "row"), P("row", "col"))
    out_specs = (P("row", "col"), P("row", "col"), P("col", "row"), P("row", "col"))
    return jax.shard_map(
        functools.partial(local, nr, nc), mesh=mesh, in_specs=in_specs, out_specs=out_specs, check_vma=False
    )
```

```python
import functools

import jax
import jax.numpy as jnp
from jax import lax
from jax.experimental import pallas as pl
from jax.experimental.pallas import tpu as pltpu
from jax.sharding import PartitionSpec as P

MESH = pl.DeviceIdType.MESH
F32, BF16 = jnp.float32, jnp.bfloat16
NN = (((1,), (0,)), ((), ()))
NT = (((1,), (1,)), ((), ()))
TN = (((0,), (0,)), ((), ()))


def cdf_of(v):
    return 0.5 * (1.0 + lax.erf(v * 0.7071067811865476))


def slope_of(v, cdf):
    return cdf + v * jnp.exp(-0.5 * v * v) * 0.3989422804014327


def cols(i, width):
    return pl.ds(pl.multiple_of(i * width, width), width)


def exchange_kernel(
    nr, nc, nck,
    past_ref, grad_ref, tok_ref, win_hbm, wout_hbm,
    xpast, xgrad, act_out, hg_out, out_lo, out_ig,
    win, wout, g_past, g_grad, g_tok, xtok, hid,
    part, pair_in, y_out, y_in, halves,
    rs_all, rs_xs, rs_xr, rs_zs, rs_zr,
    win_sem, wout_sem, up_s, up_r, dn_s, dn_r, gx_s, gx_r,
    pr_s, pr_r, y_s, y_r, hv_s, hv_r, rx_s, rx_r, rz_s, rz_r,
):
    me, col = lax.axis_index("row"), lax.axis_index("col")
    nh, ny = nr // 2, nc // 2
    h, lo = me // 2, me % 2
    g, core = col // 2, col % 2
    d, ff = win.shape
    tr = past_ref.shape[0]
    t = nr * tr
    cw, dw = ff // nck, d // nck
    partner = (h * 2 + 1 - lo, col)
    mate = (me, g * 2 + 1 - core)

    def zdev(k):
        return (k * 2 + lo, col)

    def ydev(k):
        return (me, k * 2 + core)

    def rcopy(src, dst, ss, rs, dev):
        return pltpu.make_async_remote_copy(
            src_ref=src, dst_ref=dst, send_sem=ss, recv_sem=rs, device_id=dev, device_id_type=MESH
        )

    def wout_copy(i):
        s = cols(i, cw)
        return pltpu.make_async_copy(wout_hbm.at[s, :], wout.at[s, :], wout_sem.at[i])

    def win_copy(i):
        s = cols(i, cw)
        return pltpu.make_async_copy(win_hbm.at[:, s], win.at[:, s], win_sem.at[i])

    for i in range(nck):
        wout_copy(i).start()
        win_copy(i).start()

    barrier = pltpu.get_barrier_semaphore()
    for q in range(1, nh):
        pl.semaphore_signal(barrier, inc=1, device_id=zdev((h + q) % nh), device_id_type=MESH)
    for q in range(1, ny):
        pl.semaphore_signal(barrier, inc=1, device_id=ydev((g + q) % ny), device_id_type=MESH)
    pl.semaphore_signal(barrier, inc=1, device_id=partner, device_id_type=MESH)
    pl.semaphore_signal(barrier, inc=1, device_id=mate, device_id_type=MESH)
    pl.semaphore_wait(barrier, nh + ny)

    owns = (past_ref, grad_ref, tok_ref)
    gath = (g_past, g_grad, g_tok)

    def up(a, s, src, blk):
        return rcopy(src, gath[a].at[blk], up_s.at[a, s], up_r.at[a, s], zdev(jnp.minimum(h + 1, nh - 1)))

    def down(a, s, src, blk):
        return rcopy(src, gath[a].at[blk], dn_s.at[a, s], dn_r.at[a, s], zdev(jnp.maximum(h - 1, 0)))

    def across(a, k, src, blk):
        return rcopy(src, gath[a].at[blk], gx_s.at[a, k], gx_r.at[a, k], partner)

    def start_own(a):
        across(a, h, owns[a], me).start()

        @pl.when(h < nh - 1)
        def _():
            up(a, 0, owns[a], me).start()

        @pl.when(h > 0)
        def _():
            down(a, 0, owns[a], me).start()

        gath[a][me] = owns[a][...]

    def relay(a, s):
        kb = h - 1 - s

        @pl.when(kb >= 0)
        def _():
            blk = kb * 2 + lo
            src = gath[a].at[blk]
            up(a, s, src, blk).wait_recv()

            @pl.when((h < nh - 1) & (s < nh - 2))
            def _():
                up(a, jnp.minimum(s + 1, nh - 2), src, blk).start()

            across(a, kb, src, blk).start()

        ka = h + 1 + s

        @pl.when(ka <= nh - 1)
        def _():
            blk = ka * 2 + lo
            src = gath[a].at[blk]
            down(a, s, src, blk).wait_recv()

            @pl.when((h > 0) & (s < nh - 2))
            def _():
                down(a, jnp.minimum(s + 1, nh - 2), src, blk).start()

            across(a, ka, src, blk).start()

    def collect(a, x):
        def wait_one(k, _):
            blk = k * 2 + 1 - lo
            across(a, k, gath[a].at[blk], blk).wait_recv()
            return 0

        lax.fori_loop(0, nh, wait_one, 0)

        def put(i, _):
            s = cols(i, dw)
            x[:, s] = gath[a][:, :, s].astype(F32).reshape(t, dw).astype(BF16)
            return 0

        lax.fori_loop(0, nck, put, 0)

    start_own(1)
    relay(1, 0)
    start_own(0)
    for s in range(1, nh - 1):
        relay(1, s)
    collect(1, xgrad)

    def pair_copy(a, i, half):
        return rcopy(part.at[a, i, half], pair_in.at[a, i], pr_s.at[a, i], pr_r.at[a, i], mate)

    def y_copy(a, i, q):
        return rcopy(
            y_out.at[a, i], y_in.at[a, i, q - 1], y_s.at[a, i, q - 1], y_r.at[a, i, q - 1], ydev((g + q) % ny)
        )

    def pair_add(a, j):
        pair_copy(a, j, 1 - core).wait_recv()
        total = part[a, j, core] + pair_in[a, j]
        part[a, j, core] = total
        y_out[a, j] = total.astype(BF16)

    def y_start(a, j):
        for q in range(1, ny):
            y_copy(a, j, q).start()

    def y_total(a, j):
        total = part[a, j, core]
        for q in range(1, ny):
            y_copy(a, j, q).wait_recv()
            total = total + y_in[a, j, q - 1].astype(F32)
        return total

    per = -(-(nh - 1) // nck)
    spread = max(1, nck // (nh - 1))
    lag = 2

    def finish_chunk(a, j):
        pair_add(a, j)
        y_start(a, j)

    def part_loop(a, product, behind, opens):
        def step(i, _):
            part[a, i] = product(i).reshape(2, t // 2, cw)
            pair_copy(a, i, 1 - core).start()
            if behind is not None:
                for k in range(per):
                    s = (i // spread) * per + k

                    @pl.when((i % spread == 0) & (s < nh - 1))
                    def _():
                        relay(behind, s)

            if opens is not None:
                @pl.when(i == nck // 2)
                def _():
                    start_own(opens)

            @pl.when(i >= lag)
            def _():
                finish_chunk(a, i - lag)

            return 0

        lax.fori_loop(0, nck, step, 0)

    def part_tail(a):
        def step(j, _):
            finish_chunk(a, j)
            return 0

        lax.fori_loop(nck - lag, nck, step, 0)

    def back_product(i):
        wout_copy(i).wait()
        return lax.dot_general(xgrad[...], wout[cols(i, cw), :], NT, preferred_element_type=F32)

    def past_product(i):
        win_copy(i).wait()
        return lax.dot_general(xpast[...], win[:, cols(i, cw)], NN, preferred_element_type=F32)

    def tok_product(i):
        return lax.dot_general(xtok[...], win[:, cols(i, cw)], NN, preferred_element_type=F32)

    part_loop(0, back_product, 0, 2)
    collect(0, xpast)
    part_tail(0)
    part_loop(1, past_product, 2, None)
    collect(2, xtok)
    part_tail(1)
    part_loop(2, tok_product, None, None)

    def half_copy(a, i, k):
        return rcopy(halves.at[a, i, k], halves.at[a, i, k], hv_s.at[a, i], hv_r.at[a, i], mate)

    def back_final(j, _):
        back = y_total(0, j)
        v = y_total(1, j)
        cdf = cdf_of(v)
        halves[0, j, core] = (v * cdf).astype(BF16)
        halves[1, j, core] = (back * slope_of(v, cdf)).astype(BF16)
        half_copy(1, j, core).start()
        half_copy(0, j, core).start()
        return 0

    part_tail(2)
    lax.fori_loop(0, nck, back_final, 0)

    def land(a, dst):
        def one(j, _):
            half_copy(a, j, 1 - core).wait_recv()
            dst[:, cols(j, cw)] = halves[a, j].reshape(t, cw)
            return 0

        lax.fori_loop(0, nck, one, 0)

    land(1, hg_out)

    def rx_copy(o, i):
        return rcopy(rs_xs.at[o, i], rs_xr.at[o, i], rx_s.at[o, i], rx_r.at[o, i], partner)

    def rz_copy(o, i, q):
        k = (h + q) % nh
        return rcopy(rs_zs.at[o, i, k], rs_zr.at[o, i, q - 1], rz_s.at[o, i, q - 1], rz_r.at[o, i, q - 1], zdev(k))

    rs_lag = min(4, nck - 1)

    def rs_chunk(o, j):
        rx_copy(o, j).wait_recv()
        total = rs_all[o, j, :, lo] + rs_xr[o, j].astype(F32)
        rs_all[o, j, :, lo] = total
        rs_zs[o, j] = total.astype(BF16)
        for q in range(1, nh):
            rz_copy(o, j, q).start()

    def rs_loop(o, product):
        def step(i, _):
            rs_all[o, i] = product(i).reshape(nh, 2, tr, dw)
            rs_xs[o, i] = rs_all[o, i, :, 1 - lo].astype(BF16)
            rx_copy(o, i).start()

            @pl.when(i >= rs_lag)
            def _():
                rs_chunk(o, i - rs_lag)

            return 0

        lax.fori_loop(0, nck, step, 0)

    def rs_tail(o):
        def step(j, _):
            rs_chunk(o, j)
            return 0

        lax.fori_loop(nck - rs_lag, nck, step, 0)

    rs_loop(0, lambda i: lax.dot_general(hg_out[...], win[cols(i, dw), :], NT, preferred_element_type=F32))

    def fwd_final(j, _):
        v = y_total(2, j)
        halves[2, j, core] = (v * cdf_of(v)).astype(BF16)
        half_copy(2, j, core).start()
        return 0

    lax.fori_loop(0, nck, fwd_final, 0)
    rs_tail(0)
    land(2, hid)
    rs_loop(1, lambda i: lax.dot_general(hid[...], wout[:, cols(i, dw)], NN, preferred_element_type=F32))
    land(0, act_out)
    rs_tail(1)

    def rs_final(o, out):
        def one(j, _):
            total = rs_all[o, j, h, lo]
            for q in range(1, nh):
                rz_copy(o, j, q).wait_recv()
                total = total + rs_zr[o, j, q - 1].astype(F32)
            out[:, cols(j, dw)] = total.astype(BF16)
            return 0

        lax.fori_loop(0, nck, one, 0)

    rs_final(0, out_ig)
    rs_final(1, out_lo)

    def drain(i, _):
        for a in range(3):
            pair_copy(a, i, 1 - core).wait_send()
            half_copy(a, i, core).wait_send()
            for q in range(1, ny):
                y_copy(a, i, q).wait_send()
        for o in range(2):
            rx_copy(o, i).wait_send()
            for q in range(1, nh):
                rz_copy(o, i, q).wait_send()
        return 0

    lax.fori_loop(0, nck, drain, 0)
    for a in range(3):
        def drain_across(k, _):
            across(a, k, owns[a], me).wait_send()
            return 0

        lax.fori_loop(0, nh, drain_across, 0)
        for s in range(nh - 1):
            @pl.when((h < nh - 1) & (h - s >= 0))
            def _():
                up(a, s, owns[a], me).wait_send()

            @pl.when((h > 0) & (h + s <= nh - 1))
            def _():
                down(a, s, owns[a], me).wait_send()


def grads_kernel(steps, act, grad, past, hg, lo_in, ig_in, gwo, gwi, lo_out, ig_out, so, si, sem_o, sem_i):
    lo_out[...] = lo_in[...]
    ig_out[...] = ig_in[...]
    to, ti = so.shape[0] // steps, si.shape[0] // steps

    def copy_o(i):
        return pltpu.make_async_copy(so.at[cols(i, to), :], gwo.at[cols(i, to), :], sem_o.at[i])

    def copy_i(i):
        return pltpu.make_async_copy(si.at[cols(i, ti), :], gwi.at[cols(i, ti), :], sem_i.at[i])

    def step(i, _):
        o, k = cols(i, to), cols(i, ti)
        so[o, :] = lax.dot_general(act[:, o], grad[...], TN, preferred_element_type=F32).astype(BF16)
        copy_o(i).start()
        si[k, :] = lax.dot_general(past[:, k], hg[...], TN, preferred_element_type=F32).astype(BF16)
        copy_i(i).start()
        return 0

    lax.fori_loop(0, steps, step, 0)

    def drain(i, _):
        copy_o(i).wait()
        copy_i(i).wait()
        return 0

    lax.fori_loop(0, steps, drain, 0)


def local(nr, nc, tokens, past_tokens, out_grad, w_in, w_out):
    d, ff = w_in.shape
    tr = tokens.shape[0]
    t, nh, ny, nck = nr * tr, nr // 2, nc // 2, 6
    cw, dw = ff // nck, d // nck
    dma = pltpu.SemaphoreType.DMA
    vm = pl.BlockSpec(memory_space=pltpu.VMEM)
    hbm = pl.BlockSpec(memory_space=pl.ANY)
    q = max(ny - 1, 1)
    past_all, grad_all, act_all, hg_all, lo, ig = pl.pallas_call(
        functools.partial(exchange_kernel, nr, nc, nck),
        out_shape=[
            jax.ShapeDtypeStruct((t, d), BF16),
            jax.ShapeDtypeStruct((t, d), BF16),
            jax.ShapeDtypeStruct((t, ff), BF16),
            jax.ShapeDtypeStruct((t, ff), BF16),
            jax.ShapeDtypeStruct((tr, d), BF16),
            jax.ShapeDtypeStruct((tr, d), BF16),
        ],
        in_specs=[vm, vm, vm, hbm, hbm],
        out_specs=[vm] * 6,
        scratch_shapes=[
            pltpu.VMEM((d, ff), BF16),
            pltpu.VMEM((ff, d), BF16),
            pltpu.VMEM((nr, tr, d), BF16),
            pltpu.VMEM((nr, tr, d), BF16),
            pltpu.VMEM((nr, tr, d), BF16),
            pltpu.VMEM((t, d), BF16),
            pltpu.VMEM((t, ff), BF16),
            pltpu.VMEM((3, nck, 2, t // 2, cw), F32),
            pltpu.VMEM((3, nck, t // 2, cw), F32),
            pltpu.VMEM((3, nck, t // 2, cw), BF16),
            pltpu.VMEM((3, nck, q, t // 2, cw), BF16),
            pltpu.VMEM((3, nck, 2, t // 2, cw), BF16),
            pltpu.VMEM((2, nck, nh, 2, tr, dw), F32),
            pltpu.VMEM((2, nck, nh, tr, dw), BF16),
            pltpu.VMEM((2, nck, nh, tr, dw), BF16),
            pltpu.VMEM((2, nck, nh, tr, dw), BF16),
            pltpu.VMEM((2, nck, nh - 1, tr, dw), BF16),
            dma((nck,)), dma((nck,)),
            dma((3, nh - 1)), dma((3, nh - 1)), dma((3, nh - 1)), dma((3, nh - 1)),
            dma((3, nh)), dma((3, nh)),
            dma((3, nck)), dma((3, nck)),
            dma((3, nck, q)), dma((3, nck, q)),
            dma((3, nck)), dma((3, nck)),
            dma((2, nck)), dma((2, nck)),
            dma((2, nck, nh - 1)), dma((2, nck, nh - 1)),
        ],
        compiler_params=pltpu.CompilerParams(
            collective_id=0, has_side_effects=True, vmem_limit_bytes=66 * 1000 * 1000
        ),
    )(past_tokens, out_grad, tokens, w_in, w_out)

    gwo, gwi, lo, ig = pl.pallas_call(
        functools.partial(grads_kernel, nck),
        out_shape=[
            jax.ShapeDtypeStruct((ff, d), BF16),
            jax.ShapeDtypeStruct((d, ff), BF16),
            jax.ShapeDtypeStruct((tr, d), BF16),
            jax.ShapeDtypeStruct((tr, d), BF16),
        ],
        in_specs=[vm] * 6,
        out_specs=[hbm, hbm, vm, vm],
        scratch_shapes=[pltpu.VMEM((ff, d), BF16), pltpu.VMEM((d, ff), BF16), dma((nck,)), dma((nck,))],
        cost_estimate=pl.CostEstimate(flops=4 * t * d * ff, bytes_accessed=4 * d * ff, transcendentals=0),
        compiler_params=pltpu.CompilerParams(vmem_limit_bytes=60 * 1000 * 1000),
    )(act_all, grad_all, past_all, hg_all, lo, ig)
    return lo, ig, gwi, gwo


def solution(mesh):
    nr, nc = mesh.shape["row"], mesh.shape["col"]
    in_specs = (P("row", "col"), P("row", "col"), P("row", "col"), P("col", "row"), P("row", "col"))
    out_specs = (P("row", "col"), P("row", "col"), P("col", "row"), P("row", "col"))
    return jax.shard_map(
        functools.partial(local, nr, nc), mesh=mesh, in_specs=in_specs, out_specs=out_specs, check_vma=False
    )
```
